32 devices in a mesh: tm: 16 (over z, y, x), chan: 2 (over core).
Axes of the slice: x: 2, y: 2, z: 4, core: 2. Of those that a mesh axis runs over, the one named last changes fastest.
Arguments:
- spectrum: float32 [32, 131072], P('tm', 'chan'), may hold values from -6 to 6
- offsets: int32 [64], replicated, may hold values from 0 to 16, as said below
Outputs:
- peak: float32 [131072], P('chan')
The draws below stay inside these ranges and needn't reach their ends.
Inputs may be any that keep to these rules, and one draw needn't show every extreme that they name: `offsets`: entries 0 and 1 are 0; entry 2L + d (drift d of the section that joins blocks of L) lies in 0 to L, and is exactly L for d = 2L - 1.
All inputs are finite; a program needn't handle non-finite values.
Results may differ from the reference program's by a relative error of at most 0.00002.
Values sent between devices are 32-bit elements; how exact they have to be, the bound alone decides.
A program may use at most 64 MiB of HBM per device.

```python
import jax
import jax.numpy as jnp
from jax import lax

TOTAL = 32
CHANNELS = 131072


def draw_offsets(key, part):
    count = 2 * TOTAL
    places = jnp.arange(count, dtype=jnp.int32)
    section = jnp.where(places >= 2, 1, 0).astype(jnp.int32)
    for power in range(1, 24):
        section = jnp.where(places >= 2 ** (power + 1), 2 ** power, section).astype(jnp.int32)
    drift = places - 2 * section
    jitter = jax.random.randint(jax.random.fold_in(key, 7), (count,), -1, 2).astype(jnp.int32)
    value = jnp.clip((drift + 1) // 2 + jitter, 0, section)
    value = jnp.where(drift == 2 * section - 1, section, value)
    value = jnp.where(places < 2, 0, value)
    return value.astype(jnp.int32)


def shard_levels(rng, shape, split, low, high):
    def one(axis_at, shards_of):
        draws = jax.random.uniform(jax.random.fold_in(jax.random.fold_in(rng, 6), axis_at), (shards_of,), jnp.float32, low / len(split), high / len(split))
        return jnp.repeat(jnp.exp(draws), shape[axis_at] // shards_of).reshape((-1,) + (1,) * (len(shape) - axis_at - 1))

    loudness = one(*split[0])
    for cut in split[1:]:
        loudness = loudness * one(*cut)
    return loudness


def noise(stream_key, extent, deviation, limit, cuts=(), kind=jnp.bfloat16):
    values = jax.random.normal(stream_key, extent, jnp.float32) * deviation
    if len(cuts) > 0:
        values = shard_levels(stream_key, extent, cuts, -0.22, 0.18) * values
    return jnp.clip(values, min=-limit, max=limit).astype(kind)


def setup_inputs(seed: int = 0) -> dict:
    splits = jax.random.split(jax.random.key(seed), 3)
    spectrum = noise(splits[0], (TOTAL, CHANNELS), 1.0, 6.0, ((0, 16), (1, 2)), jnp.float32)
    offsets = draw_offsets(jax.random.fold_in(splits[2], 71), 0)
    return {"spectrum": spectrum, "offsets": offsets}


def take_window(single, amount, span_cols):
    return lax.dynamic_slice_in_dim(single, amount, span_cols)


def combine(lower_rows, upper_ext, shifts, span_cols):
    upper_two = jnp.repeat(upper_ext, 2, axis=0)
    moved = jax.vmap(take_window, in_axes=(0, 0, None))(upper_two, shifts, span_cols)
    return jnp.repeat(lower_rows[:, :span_cols], 2, axis=0) + moved


def reference(spectrum, offsets):
    total = spectrum.shape[0]
    channels = spectrum.shape[1]
    sums = spectrum
    length = 1
    while length < total:
        blocks = total // (2 * length)
        paired = sums.reshape(blocks, 2, length, channels)
        lower_rows = paired[:, 0].reshape(blocks * length, channels)
        upper_rows = paired[:, 1].reshape(blocks * length, channels)
        upper_ext = jnp.pad(upper_rows, ((0, 0), (0, length)))
        shifts = jnp.tile(offsets[2 * length:4 * length], blocks).astype(jnp.int32)
        sums = combine(lower_rows, upper_ext, shifts, channels)
        length = length * 2
    return jnp.max(sums, axis=0)
```

```python
import functools

import jax
import jax.numpy as jnp
from jax import lax
from jax.experimental import pallas as pl
from jax.experimental.pallas import tpu as pltpu
from jax.sharding import PartitionSpec as P

LANES = 128
MESH = pl.DeviceIdType.MESH


def round_up(value, to):
    return (value + to - 1) // to * to


def flip(place, bits):
    out, bit = place, 1
    while bit <= bits:
        if bits & bit:
            out = out + bit * (1 - 2 * lax.rem(lax.div(place, bit), 2))
        bit *= 2
    return out


def pieces(tiles):
    if tiles % 8 or tiles < 16:
        return [(0, tiles)]
    return [(0, tiles)]


def kernel(count, chans, rows, tiles, halo, cuts, offs_hbm, x_hbm, out_ref, offs_ref, x_ref, recv, *rest):
    levels = rest[:-8]
    offs_sem, x_sem, send_sem, recv_sem, edge_sem, peak_send, peak_recv, relay_send = rest[-8:]
    me = lax.axis_index("tm")
    col = lax.axis_index("chan")
    total = count * rows
    half = count // 2
    last = len(cuts) - 1
    at_end = me == count - 1
    no_next = me * chans + col == count * chans - 1

    offs_copy = pltpu.make_async_copy(offs_hbm, offs_ref, offs_sem)
    offs_copy.start()
    x_copy = pltpu.make_async_copy(x_hbm, x_ref, x_sem)
    x_copy.start()

    barrier = pltpu.get_barrier_semaphore()
    for j in reversed(range(1, count)):
        pl.semaphore_signal(barrier, inc=1, device_id=(flip(me, j), col), device_id_type=MESH)
    if chans > 1:
        @pl.when(jnp.logical_and(at_end, col < chans - 1))
        def _():
            for t in range(count):
                pl.semaphore_signal(barrier, inc=1, device_id=(t, jnp.minimum(col + 1, chans - 1)), device_id_type=MESH)

    def extent(c):
        at, width = cuts[c]
        return at, width, width + (halo if c == 0 else 0)

    def own(c, size):
        at = cuts[c][0]
        return pltpu.make_async_copy(
            x_hbm.at[pl.ds(me * tiles + at, size)], recv.at[me, pl.ds(at, size)], recv_sem.at[c, me]
        )

    for c in range(len(cuts)):
        at, width, full = extent(c)
        if full == width:
            own(c, width).start()
        else:
            @pl.when(at_end)
            def _():
                own(c, width).start()

            @pl.when(jnp.logical_not(at_end))
            def _():
                own(c, full).start()

    x_copy.wait()
    pl.semaphore_wait(barrier, count - 1 + jnp.where(col > 0, 1, 0))

    def to_peer(c, j, size):
        k, at = flip(me, j), cuts[c][0]
        return pltpu.make_async_remote_copy(
            src_ref=x_ref.at[pl.ds(k * tiles + at, size)],
            dst_ref=recv.at[me, pl.ds(at, size)],
            send_sem=send_sem.at[c, j],
            recv_sem=recv_sem.at[c, me],
            device_id=(k, col),
            device_id_type=MESH,
        )

    def to(c, j, act):
        at, width, full = extent(c)
        if full == width:
            act(to_peer(c, j, width))
            return

        @pl.when(flip(me, j) == count - 1)
        def _():
            act(to_peer(c, j, width))

        @pl.when(flip(me, j) != count - 1)
        def _():
            act(to_peer(c, j, full))

    def edge():
        return pltpu.make_async_remote_copy(
            src_ref=x_ref.at[pl.ds(0, halo)],
            dst_ref=recv.at[me, pl.ds(tiles, halo)],
            send_sem=edge_sem.at[0],
            recv_sem=recv_sem.at[0, me],
            device_id=(count - 1, jnp.maximum(col - 1, 0)),
            device_id_type=MESH,
        )

    if chans > 1:
        @pl.when(col > 0)
        def _():
            edge().start()

    for c in range(len(cuts)):
        for j in reversed(range(1, count)):
            to(c, j, lambda copy: copy.start())

    @pl.when(no_next)
    def _():
        for t in range(count):
            recv[t, pl.ds(tiles, halo)] = jnp.zeros((halo, rows, LANES), jnp.float32)

    offs_copy.wait()

    def arrived(c, t):
        at, width, full = extent(c)

        def wait(size):
            part = recv.at[t, pl.ds(at, size)]
            pltpu.make_async_copy(part, part, recv_sem.at[c, t]).wait()

        if full == width:
            wait(width)
            return

        @pl.when(no_next)
        def _():
            wait(width)

        @pl.when(jnp.logical_not(no_next))
        def _():
            wait(full)

    def node(c, length, block, slot=0, inner=0):
        base, width, _ = extent(c)
        at = length.bit_length() - 1
        wide = width + ((total - 2 * length + LANES - 1) // LANES if c == 0 else 0)
        lane = lax.broadcasted_iota(jnp.int32, (wide, LANES), 1)

        def load(which, d, start):
            if length == 1:
                return recv[slot, pl.ds(start, wide), 2 * inner + which]
            return levels[at - 1][2 * block + which, d, pl.ds(start, wide)]

        peak = None
        for pair in range(length):
            low = load(0, pair, base)
            here = load(1, pair, base)
            ahead = load(1, pair, base + 1)

            def moved(d):
                by = offs_ref[2 * length + d]
                return pltpu.roll(jnp.where(lane >= by, here, ahead), lax.rem(LANES - by, LANES), 1)

            if 2 * length < total:
                for d in (2 * pair, 2 * pair + 1):
                    levels[at][block, d, pl.ds(base, wide)] = low + moved(d)
            else:
                value = low + jnp.maximum(moved(2 * pair), moved(2 * pair + 1))
                peak = value if peak is None else jnp.maximum(peak, value)
        return peak

    def result(c, owner, send, j):
        at, width = cuts[c]
        part = out_ref.at[pl.ds(owner * tiles + at, width)]
        return pltpu.make_async_remote_copy(
            src_ref=part,
            dst_ref=part,
            send_sem=send,
            recv_sem=peak_recv.at[c, owner],
            device_id=(flip(me, j), col),
            device_id_type=MESH,
        )

    def mine(c):
        return list(reversed(range(1, count)))

    for c in range(len(cuts)):
        peak, done = None, set()
        for j in list(range(half)) + list(reversed(range(half, count))):
            slot = flip(me, j)
            arrived(c, slot)
            done.add(j)
            length = 1
            while length < rows:
                for inner in range(rows // (2 * length)):
                    peak = node(c, length, slot * (rows // (2 * length)) + inner, slot, inner)
                length *= 2
            step = 1
            while step < count and done.issuperset(range(j // (2 * step) * 2 * step, (j // (2 * step) + 1) * 2 * step)):
                peak = node(c, step * rows, flip(lax.div(me, 2 * step), j // (2 * step)))
                step *= 2
        at, width = cuts[c]
        out_ref[pl.ds(me * tiles + at, width)] = peak
        for j in mine(c):
            result(c, me, peak_send.at[c, j], j).start()

    for c in range(0):
        owner = flip(me, half)
        result(c, owner, peak_send.at[c, half], half).wait_recv()
        for j in range(1, half):
            result(c, owner, relay_send.at[c, j], j).start()

    for c in range(len(cuts)):
        for j in range(1, count):
            to(c, j, lambda copy: copy.wait_send())
    if chans > 1:
        @pl.when(col > 0)
        def _():
            edge().wait_send()
    for c in range(len(cuts)):
        for j in mine(c):
            result(c, me, peak_send.at[c, j], j).wait_send()
        if False:
            for j in range(1, half):
                result(c, me, relay_send.at[c, j], j).wait_send()
    for c in range(len(cuts)):
        for j in range(1, count):
            if True:
                result(c, flip(me, j), peak_send.at[c, j], j).wait_recv()


def local(count, chans, spectrum, offsets):
    rows, span = spectrum.shape
    total = count * rows
    tiles = span // LANES // count
    halo = (total - 1 + LANES - 1) // LANES
    cuts = pieces(tiles)
    x = spectrum.reshape(rows, span // LANES, LANES).transpose(1, 0, 2)
    deep = round_up(tiles + halo, 8) + 8
    scratch = [
        pltpu.SMEM(offsets.shape, jnp.int32),
        pltpu.VMEM(x.shape, jnp.float32),
        pltpu.VMEM((count, deep, rows, LANES), jnp.float32),
    ]
    length = 2
    while length < total:
        scratch.append(pltpu.VMEM((total // length, length, deep, LANES), jnp.float32))
        length *= 2
    dma = pltpu.SemaphoreType.DMA
    every = dma((len(cuts), count))
    scratch += [dma, dma, every, every, dma((1,)), every, every, every]
    peak = pl.pallas_call(
        functools.partial(kernel, count, chans, rows, tiles, halo, cuts),
        out_shape=jax.ShapeDtypeStruct((count * tiles, LANES), jnp.float32),
        in_specs=[pl.BlockSpec(memory_space=pltpu.HBM), pl.BlockSpec(memory_space=pltpu.HBM)],
        out_specs=pl.BlockSpec(memory_space=pltpu.VMEM),
        scratch_shapes=scratch,
        compiler_params=pltpu.CompilerParams(collective_id=0, has_side_effects=True, vmem_limit_bytes=40 * 2**20),
    )(pltpu.with_memory_space_constraint(offsets, pltpu.HBM), pltpu.with_memory_space_constraint(x, pltpu.HBM))
    return peak.reshape(span)


def solution(mesh):
    body = functools.partial(local, mesh.shape["tm"], mesh.shape["chan"])
    placed = (P("tm", "chan"), P())
    return jax.shard_map(body, mesh=mesh, in_specs=placed, out_specs=P("chan"), check_vma=False)
```

```python
import functools

import jax
import jax.numpy as jnp
from jax import lax
from jax.experimental import pallas as pl
from jax.experimental.pallas import tpu as pltpu
from jax.sharding import PartitionSpec as P

LANES = 128
LAYERS = 4
MESH = pl.DeviceIdType.MESH


def round_up(value, to):
    return (value + to - 1) // to * to


def flip(place, bits):
    out, bit = place, 1
    while bit <= bits:
        if bits & bit:
            out = out + bit * (1 - 2 * lax.rem(lax.div(place, bit), 2))
        bit *= 2
    return out


def kernel(count, chans, rows, tiles, halo, offs_hbm, x_hbm, out_ref, offs_ref, x_ref, recv, *rest):
    levels = rest[:-9]
    offs_sem, x_sem, send_sem, recv_sem, edge_send, edge_recv, peak_send, peak_recv, known = rest[-9:]
    me = lax.axis_index("tm")
    col = lax.axis_index("chan")
    total = count * rows
    quarter = count // LAYERS
    half = 2 * quarter
    span = count * tiles
    full = tiles + halo

    offs_copy = pltpu.make_async_copy(offs_hbm, offs_ref, offs_sem)
    offs_copy.start()
    x_copy = pltpu.make_async_copy(x_hbm, x_ref.at[pl.ds(0, span)], x_sem)
    x_copy.start()

    barrier = pltpu.get_barrier_semaphore()
    for d in (3, 2, 1):
        pl.semaphore_signal(barrier, inc=1, device_id=(flip(me, d * quarter), col), device_id_type=MESH)
    for q in reversed(range(1, quarter)):
        pl.semaphore_signal(barrier, inc=1, device_id=(flip(me, q), col), device_id_type=MESH)
    if chans > 1:
        @pl.when(col < chans - 1)
        def _():
            pl.semaphore_signal(barrier, inc=1, device_id=(me, jnp.minimum(col + 1, chans - 1)), device_id_type=MESH)

    @pl.when(col == chans - 1)
    def _():
        x_ref[pl.ds(span, halo)] = jnp.zeros((halo, rows, LANES), jnp.float32)

    def own(act):
        def sized(size):
            act(
                pltpu.make_async_copy(
                    x_hbm.at[pl.ds(me * tiles, size)], recv.at[me, pl.ds(0, size)], recv_sem.at[me]
                )
            )

        @pl.when(me == count - 1)
        def _():
            sized(tiles)

        @pl.when(me != count - 1)
        def _():
            sized(full)

    def target(j):
        return flip(me, j)

    def to(j):
        k = target(j)
        return pltpu.make_async_remote_copy(
            src_ref=x_ref.at[pl.ds(k * tiles, full)],
            dst_ref=recv.at[me, pl.ds(0, full)],
            send_sem=send_sem.at[j],
            recv_sem=recv_sem.at[me],
            device_id=(k, col),
            device_id_type=MESH,
        )

    def edge():
        return pltpu.make_async_remote_copy(
            src_ref=x_ref.at[pl.ds(0, halo)],
            dst_ref=x_ref.at[pl.ds(span, halo)],
            send_sem=edge_send,
            recv_sem=edge_recv,
            device_id=(me, jnp.maximum(col - 1, 0)),
            device_id_type=MESH,
        )

    x_copy.wait()
    pl.semaphore_wait(barrier, LAYERS - 1 + quarter - 1 + jnp.where(col > 0, 1, 0))
    for q in reversed(range(1, quarter)):
        pl.semaphore_signal(known, inc=1, device_id=(flip(me, q), col), device_id_type=MESH)
    if chans > 1:
        @pl.when(col > 0)
        def _():
            edge().start()

    early = [3 * quarter, 2 * quarter]
    for j in early:
        @pl.when(target(j) != count - 1)
        def _():
            to(j).start()

    pl.semaphore_wait(known, quarter - 1)
    if chans > 1:
        @pl.when(col < chans - 1)
        def _():
            edge().wait_recv()
    for j in early:
        @pl.when(target(j) == count - 1)
        def _():
            to(j).start()
    for j in list(reversed(range(1, count))):
        if j not in early:
            to(j).start()

    own(lambda copy: copy.start())
    offs_copy.wait()

    @pl.when(me == count - 1)
    def _():
        recv[me, pl.ds(tiles, halo)] = x_ref[pl.ds(span, halo)]

    def arrived(t):
        part = recv.at[t, pl.ds(0, full)]
        pltpu.make_async_copy(part, part, recv_sem.at[t]).wait()

    def node(length, block, slot=0, part=0):
        at = length.bit_length() - 1
        wide = tiles + (total - 2 * length + LANES - 1) // LANES
        lane = lax.broadcasted_iota(jnp.int32, (wide, LANES), 1)

        def load(which, d, start):
            if length == 1:
                return recv[slot, pl.ds(start, wide), 2 * part + which]
            return levels[at - 1][2 * block + which, d, pl.ds(start, wide)]

        peak = None
        for pair in range(length):
            low = load(0, pair, 0)
            here = load(1, pair, 0)
            ahead = load(1, pair, 1)

            def moved(d):
                by = offs_ref[2 * length + d]
                return pltpu.roll(jnp.where(lane >= by, here, ahead), lax.rem(LANES - by, LANES), 1)

            if 2 * length < total:
                for d in (2 * pair, 2 * pair + 1):
                    levels[at][block, d, pl.ds(0, wide)] = low + moved(d)
            else:
                value = low + jnp.maximum(moved(2 * pair), moved(2 * pair + 1))
                peak = value if peak is None else jnp.maximum(peak, value)
        return peak

    peak, done = None, set()
    for group in [range(0, quarter), range(quarter, half), range(half, count)]:
        for j in group:
            if j:
                arrived(flip(me, j))
            else:
                own(lambda copy: copy.wait())
        done.update(group)
        length = 1
        while length < rows:
            for j in group:
                slot = flip(me, j)
                for part in range(rows // (2 * length)):
                    peak = node(length, slot * (rows // (2 * length)) + part, slot, part)
            length *= 2
        step = 1
        while step < count:
            for first in sorted({j // (2 * step) for j in group}):
                if done.issuperset(range(first * 2 * step, (first + 1) * 2 * step)):
                    peak = node(step * rows, flip(lax.div(me, 2 * step), first))
            step *= 2

    out_ref[pl.ds(me * tiles, tiles)] = peak

    def share(j, owner):
        part = out_ref.at[pl.ds(owner * tiles, tiles)]
        return pltpu.make_async_remote_copy(
            src_ref=part,
            dst_ref=part,
            send_sem=peak_send.at[j],
            recv_sem=peak_recv.at[owner],
            device_id=(flip(me, j), col),
            device_id_type=MESH,
        )

    for j in list(reversed(range(1, count))):
        share(j, me).start()
    for j in range(1, count):
        to(j).wait_send()
    if chans > 1:
        @pl.when(col > 0)
        def _():
            edge().wait_send()
    for j in list(reversed(range(1, count))):
        share(j, flip(me, j)).wait_recv()
    for j in list(reversed(range(1, count))):
        share(j, me).wait_send()


def local(count, chans, spectrum, offsets):
    rows, span = spectrum.shape
    total = count * rows
    tiles = span // LANES // count
    halo = (total - 1 + LANES - 1) // LANES
    x = spectrum.reshape(rows, span // LANES, LANES).transpose(1, 0, 2)
    deep = round_up(tiles + halo, 8) + 8
    scratch = [
        pltpu.SMEM(offsets.shape, jnp.int32),
        pltpu.VMEM((x.shape[0] + halo, rows, LANES), jnp.float32),
        pltpu.VMEM((count, deep, rows, LANES), jnp.float32),
    ]
    length = 2
    while length < total:
        scratch.append(pltpu.VMEM((total // length, length, deep, LANES), jnp.float32))
        length *= 2
    dma = pltpu.SemaphoreType.DMA
    each = dma((count,))
    scratch += [dma, dma, each, each, dma, dma, each, each, pltpu.SemaphoreType.REGULAR]
    keep = functools.partial(pltpu.with_memory_space_constraint, memory_space=pltpu.HBM)
    peak = pl.pallas_call(
        functools.partial(kernel, count, chans, rows, tiles, halo),
        out_shape=jax.ShapeDtypeStruct((count * tiles, LANES), jnp.float32),
        in_specs=[pl.BlockSpec(memory_space=pltpu.HBM), pl.BlockSpec(memory_space=pltpu.HBM)],
        out_specs=pl.BlockSpec(memory_space=pltpu.VMEM),
        scratch_shapes=scratch,
        compiler_params=pltpu.CompilerParams(collective_id=0, has_side_effects=True, vmem_limit_bytes=40 * 2**20),
    )(keep(offsets), keep(x))
    return peak.reshape(span)


def solution(mesh):
    body = functools.partial(local, mesh.shape["tm"], mesh.shape["chan"])
    placed = (P("tm", "chan"), P())
    return jax.shard_map(body, mesh=mesh, in_specs=placed, out_specs=P("chan"), check_vma=False)
```

```python
import functools

import jax
import jax.numpy as jnp
from jax import lax
from jax.experimental import pallas as pl
from jax.experimental.pallas import tpu as pltpu
from jax.sharding import PartitionSpec as P

LANES = 128
LAYERS = 4
MESH = pl.DeviceIdType.MESH


def round_up(value, to):
    return (value + to - 1) // to * to


def flip(place, bits):
    out, bit = place, 1
    while bit <= bits:
        if bits & bit:
            out = out + bit * (1 - 2 * lax.rem(lax.div(place, bit), 2))
        bit *= 2
    return out


def kernel(count, chans, rows, tiles, halo, offs_hbm, x_hbm, out_ref, offs_ref, x_ref, recv, *rest):
    levels = rest[:-9]
    offs_sem, x_sem, send_sem, recv_sem, edge_send, edge_recv, peak_send, peak_recv, known = rest[-9:]
    me = lax.axis_index("tm")
    col = lax.axis_index("chan")
    total = count * rows
    quarter = count // LAYERS
    half = 2 * quarter
    span = count * tiles
    full = tiles + halo

    offs_copy = pltpu.make_async_copy(offs_hbm, offs_ref, offs_sem)
    offs_copy.start()
    x_copy = pltpu.make_async_copy(x_hbm, x_ref.at[pl.ds(0, span)], x_sem)
    x_copy.start()

    barrier = pltpu.get_barrier_semaphore()
    for d in (3, 2, 1):
        pl.semaphore_signal(barrier, inc=1, device_id=(flip(me, d * quarter), col), device_id_type=MESH)
    for q in reversed(range(1, quarter)):
        pl.semaphore_signal(barrier, inc=1, device_id=(flip(me, q), col), device_id_type=MESH)
    if chans > 1:
        @pl.when(col < chans - 1)
        def _():
            pl.semaphore_signal(barrier, inc=1, device_id=(me, jnp.minimum(col + 1, chans - 1)), device_id_type=MESH)

    @pl.when(col == chans - 1)
    def _():
        x_ref[pl.ds(span, halo)] = jnp.zeros((halo, rows, LANES), jnp.float32)

    def own(act):
        def sized(size):
            act(
                pltpu.make_async_copy(
                    x_hbm.at[pl.ds(me * tiles, size)], recv.at[me, pl.ds(0, size)], recv_sem.at[me]
                )
            )

        @pl.when(me == count - 1)
        def _():
            sized(tiles)

        @pl.when(me != count - 1)
        def _():
            sized(full)

    def target(j):
        return flip(me, j)

    def to(j):
        k = target(j)
        return pltpu.make_async_remote_copy(
            src_ref=x_ref.at[pl.ds(k * tiles, full)],
            dst_ref=recv.at[me, pl.ds(0, full)],
            send_sem=send_sem.at[j],
            recv_sem=recv_sem.at[me],
            device_id=(k, col),
            device_id_type=MESH,
        )

    def edge():
        return pltpu.make_async_remote_copy(
            src_ref=x_ref.at[pl.ds(0, halo)],
            dst_ref=x_ref.at[pl.ds(span, halo)],
            send_sem=edge_send,
            recv_sem=edge_recv,
            device_id=(me, jnp.maximum(col - 1, 0)),
            device_id_type=MESH,
        )

    x_copy.wait()
    pl.semaphore_wait(barrier, LAYERS - 1 + quarter - 1 + jnp.where(col > 0, 1, 0))
    for q in reversed(range(1, quarter)):
        pl.semaphore_signal(known, inc=1, device_id=(flip(me, q), col), device_id_type=MESH)
    if chans > 1:
        @pl.when(col > 0)
        def _():
            edge().start()

    early = [3 * quarter, 2 * quarter]
    for j in early:
        @pl.when(target(j) != count - 1)
        def _():
            to(j).start()

    pl.semaphore_wait(known, quarter - 1)
    if chans > 1:
        @pl.when(col < chans - 1)
        def _():
            edge().wait_recv()
    for j in early:
        @pl.when(target(j) == count - 1)
        def _():
            to(j).start()
    for j in list(reversed(range(1, count))):
        if j not in early:
            to(j).start()

    own(lambda copy: copy.start())
    offs_copy.wait()

    @pl.when(me == count - 1)
    def _():
        recv[me, pl.ds(tiles, halo)] = x_ref[pl.ds(span, halo)]

    def arrived(t):
        part = recv.at[t, pl.ds(0, full)]
        pltpu.make_async_copy(part, part, recv_sem.at[t]).wait()

    def node(length, block, slot=0, part=0):
        at = length.bit_length() - 1
        wide = tiles + (total - 2 * length + LANES - 1) // LANES
        lane = lax.broadcasted_iota(jnp.int32, (wide, LANES), 1)

        def load(which, d, start):
            if length == 1:
                return recv[slot, pl.ds(start, wide), 2 * part + which]
            return levels[at - 1][2 * block + which, d, pl.ds(start, wide)]

        peak = None
        for pair in range(length):
            low = load(0, pair, 0)
            here = load(1, pair, 0)
            ahead = load(1, pair, 1)

            def moved(d):
                by = offs_ref[2 * length + d]
                return pltpu.roll(jnp.where(lane >= by, here, ahead), lax.rem(LANES - by, LANES), 1)

            if 2 * length < total:
                for d in (2 * pair, 2 * pair + 1):
                    levels[at][block, d, pl.ds(0, wide)] = low + moved(d)
            else:
                value = low + jnp.maximum(moved(2 * pair), moved(2 * pair + 1))
                peak = value if peak is None else jnp.maximum(peak, value)
        return peak

    peak, done = None, set()
    for group in [range(first, first + quarter) for first in (0, quarter, 3 * quarter, 2 * quarter)]:
        for j in group:
            if j:
                arrived(flip(me, j))
            else:
                own(lambda copy: copy.wait())
        done.update(group)
        length = 1
        while length < rows:
            for j in group:
                slot = flip(me, j)
                for part in range(rows // (2 * length)):
                    peak = node(length, slot * (rows // (2 * length)) + part, slot, part)
            length *= 2
        step = 1
        while step < count:
            for first in sorted({j // (2 * step) for j in group}):
                if done.issuperset(range(first * 2 * step, (first + 1) * 2 * step)):
                    peak = node(step * rows, flip(lax.div(me, 2 * step), first))
            step *= 2

    out_ref[pl.ds(me * tiles, tiles)] = peak

    def share(j, owner):
        part = out_ref.at[pl.ds(owner * tiles, tiles)]
        return pltpu.make_async_remote_copy(
            src_ref=part,
            dst_ref=part,
            send_sem=peak_send.at[j],
            recv_sem=peak_recv.at[owner],
            device_id=(flip(me, j), col),
            device_id_type=MESH,
        )

    def share_first():
        part = out_ref.at[pl.ds(me * tiles, tiles)]
        return pltpu.make_async_remote_copy(
            src_ref=part,
            dst_ref=part,
            send_sem=peak_send.at[me],
            recv_sem=peak_recv.at[me],
            device_id=(0, col),
            device_id_type=MESH,
        )

    @pl.when(me != 0)
    def _():
        share_first().start()

    for j in list(reversed(range(quarter, half))) + list(reversed(range(half, count))) + list(reversed(range(1, quarter))):
        @pl.when(me != j)
        def _():
            share(j, me).start()
    for j in range(1, count):
        to(j).wait_send()
    if chans > 1:
        @pl.when(col > 0)
        def _():
            edge().wait_send()
    for j in list(reversed(range(1, count))):
        share(j, flip(me, j)).wait_recv()
    for j in list(reversed(range(1, count))):
        share(j, me).wait_send()


def local(count, chans, spectrum, offsets):
    rows, span = spectrum.shape
    total = count * rows
    tiles = span // LANES // count
    halo = (total - 1 + LANES - 1) // LANES
    x = spectrum.reshape(rows, span // LANES, LANES).transpose(1, 0, 2)
    deep = round_up(tiles + halo, 8) + 8
    scratch = [
        pltpu.SMEM(offsets.shape, jnp.int32),
        pltpu.VMEM((x.shape[0] + halo, rows, LANES), jnp.float32),
        pltpu.VMEM((count, deep, rows, LANES), jnp.float32),
    ]
    length = 2
    while length < total:
        scratch.append(pltpu.VMEM((total // length, length, deep, LANES), jnp.float32))
        length *= 2
    dma = pltpu.SemaphoreType.DMA
    each = dma((count,))
    scratch += [dma, dma, each, each, dma, dma, each, each, pltpu.SemaphoreType.REGULAR]
    keep = functools.partial(pltpu.with_memory_space_constraint, memory_space=pltpu.HBM)
    peak = pl.pallas_call(
        functools.partial(kernel, count, chans, rows, tiles, halo),
        out_shape=jax.ShapeDtypeStruct((count * tiles, LANES), jnp.float32),
        in_specs=[pl.BlockSpec(memory_space=pltpu.HBM), pl.BlockSpec(memory_space=pltpu.HBM)],
        out_specs=pl.BlockSpec(memory_space=pltpu.VMEM),
        scratch_shapes=scratch,
        compiler_params=pltpu.CompilerParams(collective_id=0, has_side_effects=True, vmem_limit_bytes=40 * 2**20),
    )(keep(offsets), keep(x))
    return peak.reshape(span)


def solution(mesh):
    body = functools.partial(local, mesh.shape["tm"], mesh.shape["chan"])
    placed = (P("tm", "chan"), P())
    return jax.shard_map(body, mesh=mesh, in_specs=placed, out_specs=P("chan"), check_vma=False)
```

```python
import functools

import jax
import jax.numpy as jnp
from jax import lax
from jax.experimental import pallas as pl
from jax.experimental.pallas import tpu as pltpu
from jax.sharding import PartitionSpec as P

LANES = 128
LAYERS = 4
MESH = pl.DeviceIdType.MESH


def round_up(value, to):
    return (value + to - 1) // to * to


def flip(place, bits):
    out, bit = place, 1
    while bit <= bits:
        if bits & bit:
            out = out + bit * (1 - 2 * lax.rem(lax.div(place, bit), 2))
        bit *= 2
    return out


def kernel(count, chans, rows, tiles, halo, offs_hbm, x_hbm, out_ref, offs_ref, x_ref, recv, *rest):
    levels = rest[:-9]
    offs_sem, x_sem, send_sem, recv_sem, edge_send, edge_recv, peak_send, peak_recv, known = rest[-9:]
    me = lax.axis_index("tm")
    col = lax.axis_index("chan")
    total = count * rows
    quarter = count // LAYERS
    half = 2 * quarter
    span = count * tiles
    full = tiles + halo

    offs_copy = pltpu.make_async_copy(offs_hbm, offs_ref, offs_sem)
    offs_copy.start()
    x_copy = pltpu.make_async_copy(x_hbm, x_ref.at[pl.ds(0, span)], x_sem)
    x_copy.start()

    barrier = pltpu.get_barrier_semaphore()
    for d in (3, 2, 1):
        pl.semaphore_signal(barrier, inc=1, device_id=(flip(me, d * quarter), col), device_id_type=MESH)
    for q in reversed(range(1, quarter)):
        pl.semaphore_signal(barrier, inc=1, device_id=(flip(me, q), col), device_id_type=MESH)
    if chans > 1:
        @pl.when(col < chans - 1)
        def _():
            pl.semaphore_signal(barrier, inc=1, device_id=(me, jnp.minimum(col + 1, chans - 1)), device_id_type=MESH)

    @pl.when(col == chans - 1)
    def _():
        x_ref[pl.ds(span, halo)] = jnp.zeros((halo, rows, LANES), jnp.float32)

    def own(act):
        def sized(size):
            act(
                pltpu.make_async_copy(
                    x_hbm.at[pl.ds(me * tiles, size)], recv.at[me, pl.ds(0, size)], recv_sem.at[me]
                )
            )

        @pl.when(me == count - 1)
        def _():
            sized(tiles)

        @pl.when(me != count - 1)
        def _():
            sized(full)

    def target(j):
        return flip(me, j)

    def to(j):
        k = target(j)
        return pltpu.make_async_remote_copy(
            src_ref=x_ref.at[pl.ds(k * tiles, full)],
            dst_ref=recv.at[me, pl.ds(0, full)],
            send_sem=send_sem.at[j],
            recv_sem=recv_sem.at[me],
            device_id=(k, col),
            device_id_type=MESH,
        )

    def edge():
        return pltpu.make_async_remote_copy(
            src_ref=x_ref.at[pl.ds(0, halo)],
            dst_ref=x_ref.at[pl.ds(span, halo)],
            send_sem=edge_send,
            recv_sem=edge_recv,
            device_id=(me, jnp.maximum(col - 1, 0)),
            device_id_type=MESH,
        )

    x_copy.wait()
    pl.semaphore_wait(barrier, LAYERS - 1 + quarter - 1 + jnp.where(col > 0, 1, 0))
    for q in reversed(range(1, quarter)):
        pl.semaphore_signal(known, inc=1, device_id=(flip(me, q), col), device_id_type=MESH)
    if chans > 1:
        @pl.when(col > 0)
        def _():
            edge().start()

    early = [3 * quarter, 2 * quarter]
    for j in early:
        @pl.when(target(j) != count - 1)
        def _():
            to(j).start()

    pl.semaphore_wait(known, quarter - 1)
    if chans > 1:
        @pl.when(col < chans - 1)
        def _():
            edge().wait_recv()
    for j in early:
        @pl.when(target(j) == count - 1)
        def _():
            to(j).start()
    for j in list(reversed(range(1, count))):
        if j not in early:
            to(j).start()

    own(lambda copy: copy.start())
    offs_copy.wait()

    @pl.when(me == count - 1)
    def _():
        recv[me, pl.ds(tiles, halo)] = x_ref[pl.ds(span, halo)]

    def arrived(t):
        part = recv.at[t, pl.ds(0, full)]
        pltpu.make_async_copy(part, part, recv_sem.at[t]).wait()

    def node(length, block, slot=0, part=0):
        at = length.bit_length() - 1
        wide = tiles + (total - 2 * length + LANES - 1) // LANES
        lane = lax.broadcasted_iota(jnp.int32, (wide, LANES), 1)

        def load(which, d, start):
            if length == 1:
                return recv[slot, pl.ds(start, wide), 2 * part + which]
            return levels[at - 1][2 * block + which, d, pl.ds(start, wide)]

        peak = None
        for pair in range(length):
            low = load(0, pair, 0)
            here = load(1, pair, 0)
            ahead = load(1, pair, 1)

            def moved(d):
                by = offs_ref[2 * length + d]
                return pltpu.roll(jnp.where(lane >= by, here, ahead), lax.rem(LANES - by, LANES), 1)

            if 2 * length < total:
                for d in (2 * pair, 2 * pair + 1):
                    levels[at][block, d, pl.ds(0, wide)] = low + moved(d)
            else:
                value = low + jnp.maximum(moved(2 * pair), moved(2 * pair + 1))
                peak = value if peak is None else jnp.maximum(peak, value)
        return peak

    peak, done = None, set()
    for group in [range(0, half), range(half + quarter, count), range(half, half + quarter)]:
        for j in group:
            if j:
                arrived(flip(me, j))
            else:
                own(lambda copy: copy.wait())
        done.update(group)
        length = 1
        while length < rows:
            for j in group:
                slot = flip(me, j)
                for part in range(rows // (2 * length)):
                    peak = node(length, slot * (rows // (2 * length)) + part, slot, part)
            length *= 2
        step = 1
        while step < count:
            for first in sorted({j // (2 * step) for j in group}):
                if done.issuperset(range(first * 2 * step, (first + 1) * 2 * step)):
                    peak = node(step * rows, flip(lax.div(me, 2 * step), first))
            step *= 2

    out_ref[pl.ds(me * tiles, tiles)] = peak

    def share(j, owner):
        part = out_ref.at[pl.ds(owner * tiles, tiles)]
        return pltpu.make_async_remote_copy(
            src_ref=part,
            dst_ref=part,
            send_sem=peak_send.at[j],
            recv_sem=peak_recv.at[owner],
            device_id=(flip(me, j), col),
            device_id_type=MESH,
        )

    def share_first():
        part = out_ref.at[pl.ds(me * tiles, tiles)]
        return pltpu.make_async_remote_copy(
            src_ref=part,
            dst_ref=part,
            send_sem=peak_send.at[me],
            recv_sem=peak_recv.at[me],
            device_id=(0, col),
            device_id_type=MESH,
        )

    @pl.when(me != 0)
    def _():
        share_first().start()

    for j in list(reversed(range(quarter, half))) + list(reversed(range(half, count))) + list(reversed(range(1, quarter))):
        @pl.when(me != j)
        def _():
            share(j, me).start()
    for j in range(1, count):
        to(j).wait_send()
    if chans > 1:
        @pl.when(col > 0)
        def _():
            edge().wait_send()
    for j in list(reversed(range(1, count))):
        share(j, flip(me, j)).wait_recv()
    for j in list(reversed(range(1, count))):
        share(j, me).wait_send()


def local(count, chans, spectrum, offsets):
    rows, span = spectrum.shape
    total = count * rows
    tiles = span // LANES // count
    halo = (total - 1 + LANES - 1) // LANES
    x = spectrum.reshape(rows, span // LANES, LANES).transpose(1, 0, 2)
    deep = round_up(tiles + halo, 8) + 8
    scratch = [
        pltpu.SMEM(offsets.shape, jnp.int32),
        pltpu.VMEM((x.shape[0] + halo, rows, LANES), jnp.float32),
        pltpu.VMEM((count, deep, rows, LANES), jnp.float32),
    ]
    length = 2
    while length < total:
        scratch.append(pltpu.VMEM((total // length, length, deep, LANES), jnp.float32))
        length *= 2
    dma = pltpu.SemaphoreType.DMA
    each = dma((count,))
    scratch += [dma, dma, each, each, dma, dma, each, each, pltpu.SemaphoreType.REGULAR]
    keep = functools.partial(pltpu.with_memory_space_constraint, memory_space=pltpu.HBM)
    peak = pl.pallas_call(
        functools.partial(kernel, count, chans, rows, tiles, halo),
        out_shape=jax.ShapeDtypeStruct((count * tiles, LANES), jnp.float32),
        in_specs=[pl.BlockSpec(memory_space=pltpu.HBM), pl.BlockSpec(memory_space=pltpu.HBM)],
        out_specs=pl.BlockSpec(memory_space=pltpu.VMEM),
        scratch_shapes=scratch,
        compiler_params=pltpu.CompilerParams(collective_id=0, has_side_effects=True, vmem_limit_bytes=40 * 2**20),
    )(keep(offsets), keep(x))
    return peak.reshape(span)


def solution(mesh):
    body = functools.partial(local, mesh.shape["tm"], mesh.shape["chan"])
    placed = (P("tm", "chan"), P())
    return jax.shard_map(body, mesh=mesh, in_specs=placed, out_specs=P("chan"), check_vma=False)
```
